8 devices in a mesh: dp: 1 (over z), col: 2 (over y), row: 4 (over x, core).
Axes of the slice: x: 2, y: 2, z: 1, core: 2. Of those that a mesh axis runs over, the one named last changes fastest.
Arguments:
- hidden: bfloat16 [64, 4096], P('dp', 'row')
- norm_gain: float32 [4096], P('row')
- w_head: bfloat16 [4096, 32768], P('row', 'col')
Outputs:
- output 1: float32 [64, 32768], P('dp', ('col', 'row'))
- output 2: float32 [64], P('dp')
All inputs are finite; a program needn't handle non-finite values.
Results may differ from the reference program's by a relative error of at most 0.001.
Values sent between devices are 32-bit elements.
A program may use at most 1 GiB of HBM per device.

```python
import jax
import jax.numpy as jnp
from jax import lax

BATCH = 64
HIDDEN = 4096
VOCAB = 32768
EPS = 1e-5


def setup_inputs(seed: int = 0, part: int = 0) -> dict:
    key = jax.random.key(seed)
    part_key = jax.random.fold_in(key, part)
    key_tok, key_feat = jax.random.split(part_key, 2)
    key_gain, key_weight = jax.random.split(key, 2)
    position = jnp.arange(HIDDEN, dtype=jnp.float32) / HIDDEN
    feat_scale = (0.4 + 1.2 * position) * jax.random.uniform(key_feat, (HIDDEN,), jnp.float32, 0.8, 1.2)
    hidden = jax.random.normal(key_tok, (BATCH, HIDDEN), jnp.float32) * feat_scale
    gain = 2.4 / (0.4 + 1.2 * position) * jax.random.uniform(key_gain, (HIDDEN,), jnp.float32, 0.7, 1.3)
    weight = jax.random.normal(key_weight, (HIDDEN, VOCAB), jnp.float32) * HIDDEN ** -0.5
    return {"hidden": hidden.astype(jnp.bfloat16), "norm_gain": gain, "w_head": weight.astype(jnp.bfloat16)}


def reference(hidden, norm_gain, w_head):
    wide_hidden = hidden.astype(jnp.float32)
    mean_sq = jnp.mean(wide_hidden * wide_hidden, axis=-1, keepdims=True)
    normed = (wide_hidden * lax.rsqrt(mean_sq + EPS) * norm_gain).astype(jnp.bfloat16)
    logits = jnp.dot(normed, w_head, preferred_element_type=jnp.float32)
    log_norm = jax.nn.logsumexp(logits, axis=-1)
    return logits - log_norm[:, None], log_norm
```

```python
import functools

import jax
import jax.numpy as jnp
from jax import lax
from jax.experimental import pallas as pl
from jax.experimental.pallas import tpu as pltpu
from jax.sharding import PartitionSpec as P

EPS = 1e-5
MESH = pl.DeviceIdType.MESH
LANES = 128
TILE = 256
IN_FLIGHT = 8


def head_kernel(
    hidden_total,
    hidden_ref,
    gain_ref,
    w_ref,
    logits_ref,
    lse_ref,
    col_ref,
    w_buf,
    x_buf,
    sq_send,
    sq_recv,
    pair_send,
    pair_recv,
    cross_send,
    cross_recv,
    mass_send,
    mass_recv,
    max_acc,
    sum_acc,
    w_sem,
    sq_ssem,
    sq_rsem,
    pair_ssem,
    pair_rsem,
    cross_ssem,
    cross_rsem,
    mass_ssem,
    mass_rsem,
):
    dp = lax.axis_index("dp")
    col = lax.axis_index("col")
    row = lax.axis_index("row")
    core = row % 2
    chip = row // 2
    partner = chip * 2 + (1 - core)
    across = (1 - chip) * 2 + core
    diagonal = (1 - chip) * 2 + (1 - core)
    row_peers = [(col, partner), (col, across), (col, diagonal)]
    other = 1 - col
    col_peers = [(other, row), (other, partner), (other, across), (other, diagonal)]
    peers = row_peers + col_peers

    batch = hidden_ref.shape[0]
    block = logits_ref.shape[1]
    tiles = block // TILE

    def where(peer):
        return (dp, peer[0], peer[1])

    barrier = pltpu.get_barrier_semaphore()
    for peer in peers:
        pl.semaphore_signal(barrier, inc=1, device_id=where(peer), device_id_type=MESH)

    def w_copy(k):
        phase = k // (2 * tiles)
        mine = k % 2
        index = (k % (2 * tiles)) // 2
        target_chip = (1 - phase) * (1 - chip) + phase * chip
        target_core = mine * core + (1 - mine) * (1 - core)
        target = target_chip * 2 + target_core
        start = pl.multiple_of(target * block + index * TILE, TILE)
        return pltpu.make_async_copy(w_ref.at[:, pl.ds(start, TILE)], w_buf.at[k], w_sem.at[k])

    def issue(k, carry):
        w_copy(k).start()
        return carry

    lax.fori_loop(0, IN_FLIGHT, issue, 0)

    wide = hidden_ref[...].astype(jnp.float32)
    local_sq = jnp.sum(wide * wide, axis=-1, keepdims=True)
    sq_send[...] = jnp.broadcast_to(local_sq, sq_send.shape)

    pl.semaphore_wait(barrier, len(peers))

    sq_copies = []
    for n, peer in enumerate(row_peers):
        copy = pltpu.make_async_remote_copy(
            src_ref=sq_send,
            dst_ref=sq_recv.at[n],
            send_sem=sq_ssem.at[n],
            recv_sem=sq_rsem.at[n],
            device_id=where(peer),
            device_id_type=MESH,
        )
        copy.start()
        sq_copies.append(copy)
    for copy in sq_copies:
        copy.wait()
    pair_here = sq_send[...] + sq_recv[0]
    pair_there = sq_recv[1] + sq_recv[2]
    total_sq = (pair_here + pair_there)[:, :1]
    inv = lax.rsqrt(total_sq / hidden_total + EPS)
    x_buf[...] = (wide * inv * gain_ref[...]).astype(jnp.bfloat16)

    def product(k):
        w_copy(k).wait()

        @pl.when(k + IN_FLIGHT < 4 * tiles)
        def _():
            w_copy(k + IN_FLIGHT).start()

        return jnp.dot(x_buf[...], w_buf[k], preferred_element_type=jnp.float32)

    def pair_copy(n):
        return pltpu.make_async_remote_copy(
            src_ref=pair_send.at[n],
            dst_ref=pair_recv.at[n],
            send_sem=pair_ssem.at[n],
            recv_sem=pair_rsem.at[n],
            device_id=where((col, partner)),
            device_id_type=MESH,
        )

    def cross_copy(n):
        return pltpu.make_async_remote_copy(
            src_ref=cross_send.at[n],
            dst_ref=cross_recv.at[n],
            send_sem=cross_ssem.at[n],
            recv_sem=cross_rsem.at[n],
            device_id=where((col, across)),
            device_id_type=MESH,
        )

    def outgoing(n, carry):
        pair_send[n] = product(2 * n)
        pair_copy(n).start()
        own = product(2 * n + 1)
        pair_copy(n).wait_recv()
        cross_send[n] = own + pair_recv[n]
        cross_copy(n).start()
        return carry

    lax.fori_loop(0, tiles, outgoing, 0)

    def local(n, carry):
        k = tiles + n
        pair_send[k] = product(2 * k)
        pair_copy(k).start()
        own = product(2 * k + 1)
        pair_copy(k).wait_recv()
        logits_ref[:, pl.ds(pl.multiple_of(n * TILE, TILE), TILE)] = own + pair_recv[k]
        return carry

    lax.fori_loop(0, tiles, local, 0)

    max_acc[...] = jnp.full(max_acc.shape, -jnp.inf, jnp.float32)
    sum_acc[...] = jnp.zeros(sum_acc.shape, jnp.float32)

    def finish(n, carry):
        cross_copy(n).wait_recv()
        columns = pl.ds(pl.multiple_of(n * TILE, TILE), TILE)
        z = logits_ref[:, columns] + cross_recv[n]
        logits_ref[:, columns] = z
        pieces = [z[:, i * LANES : (i + 1) * LANES] for i in range(TILE // LANES)]
        high = functools.reduce(jnp.maximum, pieces, max_acc[...])
        mass = sum_acc[...] * jnp.exp(max_acc[...] - high)
        for piece in pieces:
            mass = mass + jnp.exp(piece - high)
        max_acc[...] = high
        sum_acc[...] = mass
        return carry

    lax.fori_loop(0, tiles, finish, 0)

    high_t = max_acc[...].T
    mass_t = sum_acc[...].T
    high = jnp.max(high_t, axis=0, keepdims=True)
    mass = jnp.sum(mass_t * jnp.exp(high_t - high), axis=0, keepdims=True)
    mass_send[0:1, :] = high
    mass_send[1:2, :] = mass

    mass_copies = []
    for n, peer in enumerate(peers):
        copy = pltpu.make_async_remote_copy(
            src_ref=mass_send,
            dst_ref=mass_recv.at[n],
            send_sem=mass_ssem.at[n],
            recv_sem=mass_rsem.at[n],
            device_id=where(peer),
            device_id_type=MESH,
        )
        copy.start()
        mass_copies.append(copy)
    for n in range(2 * tiles):
        pair_copy(n).wait_send()
    for n in range(tiles):
        cross_copy(n).wait_send()
    for copy in mass_copies:
        copy.wait()
    highs = [high] + [mass_recv[n, 0:1, :] for n in range(len(peers))]
    masses = [mass] + [mass_recv[n, 1:2, :] for n in range(len(peers))]
    top = functools.reduce(jnp.maximum, highs)
    terms = [m * jnp.exp(h - top) for h, m in zip(highs, masses)]
    here = (terms[0] + terms[1]) + (terms[2] + terms[3])
    there = (terms[4] + terms[5]) + (terms[6] + terms[7])
    lse = top + jnp.log(here + there)
    lse_ref[...] = lse
    col_ref[...] = jnp.broadcast_to(lse, (LANES, batch)).T


def solution(mesh):
    row_count = mesh.shape["row"]

    def local_head(hidden, norm_gain, w_head):
        batch, depth = hidden.shape
        block = w_head.shape[1] // row_count
        tiles = block // TILE
        peer_count = 7
        logits, lse, lse_col = pl.pallas_call(
            functools.partial(head_kernel, float(depth * row_count)),
            out_shape=(
                jax.ShapeDtypeStruct((batch, block), jnp.float32),
                jax.ShapeDtypeStruct((1, batch), jnp.float32),
                jax.ShapeDtypeStruct((batch, LANES), jnp.float32),
            ),
            in_specs=[
                pl.BlockSpec(memory_space=pltpu.VMEM),
                pl.BlockSpec(memory_space=pltpu.VMEM),
                pl.BlockSpec(memory_space=pl.ANY),
            ],
            out_specs=(
                pl.BlockSpec(memory_space=pltpu.VMEM),
                pl.BlockSpec(memory_space=pltpu.VMEM),
                pl.BlockSpec(memory_space=pltpu.VMEM),
            ),
            scratch_shapes=[
                pltpu.VMEM((4 * tiles, depth, TILE), jnp.bfloat16),
                pltpu.VMEM((batch, depth), jnp.bfloat16),
                pltpu.VMEM((batch, LANES), jnp.float32),
                pltpu.VMEM((3, batch, LANES), jnp.float32),
                pltpu.VMEM((2 * tiles, batch, TILE), jnp.float32),
                pltpu.VMEM((2 * tiles, batch, TILE), jnp.float32),
                pltpu.VMEM((tiles, batch, TILE), jnp.float32),
                pltpu.VMEM((tiles, batch, TILE), jnp.float32),
                pltpu.VMEM((2, batch), jnp.float32),
                pltpu.VMEM((peer_count, 2, batch), jnp.float32),
                pltpu.VMEM((batch, LANES), jnp.float32),
                pltpu.VMEM((batch, LANES), jnp.float32),
                pltpu.SemaphoreType.DMA((4 * tiles,)),
                pltpu.SemaphoreType.DMA((3,)),
                pltpu.SemaphoreType.DMA((3,)),
                pltpu.SemaphoreType.DMA((2 * tiles,)),
                pltpu.SemaphoreType.DMA((2 * tiles,)),
                pltpu.SemaphoreType.DMA((tiles,)),
                pltpu.SemaphoreType.DMA((tiles,)),
                pltpu.SemaphoreType.DMA((peer_count,)),
                pltpu.SemaphoreType.DMA((peer_count,)),
            ],
            compiler_params=pltpu.CompilerParams(
                collective_id=0, has_side_effects=True, vmem_limit_bytes=56 * 1024 * 1024
            ),
        )(hidden, norm_gain.reshape(1, depth), w_head)
        return logits - lse_col[:, :1], lse[0]

    return jax.shard_map(
        local_head,
        mesh=mesh,
        in_specs=(P("dp", "row"), P("row"), P("row", "col")),
        out_specs=(P("dp", ("col", "row")), P("dp")),
        check_vma=False,
    )
```
